32 devices in a mesh: rows: 16 (over z, x, core), cols: 2 (over y).
Axes of the slice: x: 2, y: 2, z: 4, core: 2. Of those that a mesh axis runs over, the one named last changes fastest.
Arguments:
- current_frame: bfloat16 [128, 256, 256], P(None, 'rows', 'cols'), may hold values from -6 to 6
- history_frames: bfloat16 [3, 128, 256, 256], P(None, None, 'rows', 'cols'), may hold values from -6 to 6
- offsets: int32 [3, 2], replicated, may hold values from -16 to 16, as said below
- compress_weight: bfloat16 [32, 128], replicated, may hold values from -0.5 to 0.5
- mixer_weight: bfloat16 [3, 3, 128, 224], replicated, may hold values from -0.125 to 0.125
- mixer_bias: float32 [128], replicated, may hold values from -3 to 3
Outputs:
- joined_grid: bfloat16 [128, 256, 256], P(None, 'rows', 'cols')
The draws below stay inside these ranges and needn't reach their ends.
Inputs may be any that keep to these rules, and one draw needn't show every extreme that they name: offsets[k, 0] lies in -8..8 and offsets[k, 1] in -16..16; no offset is 0; in each of the two columns one frame's offset equals the bound and another equals its negative.
All inputs are finite; a program needn't handle non-finite values.
Results may differ from the reference program's by a relative error of at most 0.0034.
Values may be sent and summed in bfloat16 or wider, within the bound.
A program may use at most 64 MiB of HBM per device.

```python
import jax
import jax.numpy as jnp
from jax import lax

C = 128
CP = 32
FRAMES = 3
CR = 16
SHIFT_X = 16
SHIFT_Y = 8
GRID_ROWS = 256
GRID_COLS = 256


def offset_column(key, bound):
    key_mags, key_sign, key_perm = jax.random.split(key, 3)
    spare_mag = jax.random.randint(key_mags, (), 1, bound + 1)
    mags = jnp.stack([jnp.int32(bound), jnp.int32(bound), spare_mag.astype(jnp.int32)])
    spare = 2 * jax.random.randint(key_sign, (), 0, 2) - 1
    signs = jnp.stack([jnp.int32(1), jnp.int32(-1), spare.astype(jnp.int32)])
    order = jax.random.permutation(key_perm, jnp.arange(3, dtype=jnp.int32))
    return (mags * signs)[order]


def draw_offsets(key, part):
    key_rows = jax.random.fold_in(key, 11)
    key_cols = jax.random.fold_in(key, 23)
    return jnp.stack([offset_column(key_rows, SHIFT_Y), offset_column(key_cols, SHIFT_X)], axis=1).astype(jnp.int32)


def block_scale(stream_key, extent, shards, low, largest):
    gain = 1.0
    for axis_at, parts in shards:
        draws = jax.random.uniform(jax.random.fold_in(jax.random.fold_in(stream_key, 6), axis_at), (parts,), jnp.float32, low / len(shards), largest / len(shards))
        gain = gain * jnp.repeat(jnp.exp(draws), extent[axis_at] // parts).reshape((-1,) + (1,) * (len(extent) - 1 - axis_at))
    return gain


def noise(key, dims, scale, reach, cuts=(), kind=jnp.bfloat16):
    drawn = scale * jax.random.normal(key, dims, jnp.float32)
    if cuts:
        drawn = drawn * block_scale(key, dims, cuts, -0.22, 0.18)
    return jnp.clip(drawn, -reach, reach).astype(kind)


def setup_inputs(seed: int = 0) -> dict:
    key_list = jax.random.split(jax.random.key(seed), 7)
    return {
        "current_frame": noise(key_list[0], (C, GRID_ROWS, GRID_COLS), 1.0, 6.0, ((1, 16), (2, 2))),
        "history_frames": noise(key_list[1], (FRAMES, C, GRID_ROWS, GRID_COLS), 1.0, 6.0, ((2, 16), (3, 2))),
        "offsets": draw_offsets(jax.random.fold_in(key_list[6], 71), 0),
        "compress_weight": noise(key_list[3], (CP, C), C ** -0.5, 0.5),
        "mixer_weight": noise(key_list[4], (3, 3, C, C + FRAMES * CP), (9 * (C + FRAMES * CP)) ** -0.5, 0.125),
        "mixer_bias": noise(key_list[5], (C,), 0.5, 3.0, (), jnp.float32),
    }


def shift_frame(frame, row_offset, col_offset):
    padded = jnp.pad(frame, ((0, 0), (SHIFT_Y, SHIFT_Y), (SHIFT_X, SHIFT_X)))
    starts = (jnp.int32(0), (SHIFT_Y - row_offset).astype(jnp.int32), (SHIFT_X - col_offset).astype(jnp.int32))
    return lax.dynamic_slice(padded, starts, (CP, GRID_ROWS, GRID_COLS))


def conv_taps(present_rows, older_rows, mixer_weight, mixer_bias):
    height = present_rows.shape[1] - 2
    width = present_rows.shape[2] - 2
    channels = present_rows.shape[0]
    total = jnp.zeros((mixer_weight.shape[2], height * width), jnp.float32)
    for tap_row in range(3):
        for tap_col in range(3):
            present = present_rows[:, tap_row:tap_row + height, tap_col:tap_col + width].reshape(channels, -1)
            older = older_rows[:, tap_row:tap_row + height, tap_col:tap_col + width].reshape(older_rows.shape[0], -1)
            total = total + jnp.dot(mixer_weight[tap_row, tap_col, :, :channels], present, preferred_element_type=jnp.float32)
            total = total + jnp.dot(mixer_weight[tap_row, tap_col, :, channels:], older, preferred_element_type=jnp.float32)
    result = jnp.maximum(total + mixer_bias[:, None], 0.0)
    return result.astype(jnp.bfloat16).reshape(-1, height, width)


def reference(current_frame, history_frames, offsets, compress_weight, mixer_weight, mixer_bias):
    pieces = []
    for frame_index in range(FRAMES):
        flattened = history_frames[frame_index].reshape(C, -1)
        reduced = jnp.dot(compress_weight, flattened, preferred_element_type=jnp.float32).astype(jnp.bfloat16)
        reduced = reduced.reshape(CP, GRID_ROWS, GRID_COLS)
        pieces.append(shift_frame(reduced, offsets[frame_index, 0], offsets[frame_index, 1]))
    shifted = jnp.concatenate(pieces, axis=0)
    present_pad = jnp.pad(current_frame, ((0, 0), (1, 1), (1, 1)))
    older_pad = jnp.pad(shifted, ((0, 0), (1, 1), (1, 1)))

    def row_block(block_index):
        row_start = (block_index * CR).astype(jnp.int32)
        present_rows = lax.dynamic_slice_in_dim(present_pad, row_start, CR + 2, 1)
        older_rows = lax.dynamic_slice_in_dim(older_pad, row_start, CR + 2, 1)
        return conv_taps(present_rows, older_rows, mixer_weight, mixer_bias)

    blocks = lax.map(row_block, jnp.arange(GRID_ROWS // CR, dtype=jnp.int32))
    return blocks.transpose(1, 0, 2, 3).reshape(C, GRID_ROWS, GRID_COLS)
```

```python
import jax
import jax.numpy as jnp
from jax import lax
from jax.sharding import PartitionSpec as P

CP = 32
SHIFT_X = 16
SPLIT = True


def exchange(first, last, axis):
    size = lax.axis_size(axis)
    up = [(i, (i + 1) % size) for i in range(size - 1)]
    down = [(j, i) for i, j in up]
    return lax.ppermute(last, axis, up), lax.ppermute(first, axis, down)


def widen(block, rows, channels):
    return jnp.pad(block, ((0, rows - block.shape[0]), (0, 0), (0, channels - block.shape[2])))


def conv(block, weight):
    return lax.conv_general_dilated(
        block[None],
        weight,
        (1, 1),
        "VALID",
        dimension_numbers=("NHWC", "HWOI", "NHWC"),
        preferred_element_type=jnp.float32,
    )[0]


def body(current_frame, history_frames, offsets, compress_weight, mixer_weight, mixer_bias):
    frames, channels, height, width = history_frames.shape
    depth = frames * CP
    reach_rows = height // 2 + 1
    reach_cols = SHIFT_X + 1
    reduced = jnp.einsum(
        "oc,fcrx->rfox", compress_weight, history_frames, preferred_element_type=jnp.float32
    ).astype(jnp.bfloat16)
    source = reduced.reshape(height, depth, width).transpose(0, 2, 1)
    present = current_frame.transpose(1, 2, 0)
    wide = max(depth, channels)

    def row_pack(own, now):
        return jnp.concatenate([widen(own, reach_rows, wide), widen(now, 1, wide)], axis=0)

    above, below = exchange(
        row_pack(source[:reach_rows], present[:1]),
        row_pack(source[height - reach_rows :], present[height - 1 :]),
        "rows",
    )
    source = jnp.concatenate(
        [above[:reach_rows, :, :depth], source, below[:reach_rows, :, :depth]], axis=0
    )
    present = jnp.concatenate(
        [above[reach_rows:, :, :channels], present, below[reach_rows:, :, :channels]], axis=0
    )
    span = source.shape[0]

    def col_pack(own, now):
        return jnp.concatenate([widen(own, span, wide), widen(now, span, wide)], axis=1)

    left, right = exchange(
        col_pack(source[:, :reach_cols], present[:, :1]),
        col_pack(source[:, width - reach_cols :], present[:, width - 1 :]),
        "cols",
    )
    source = jnp.concatenate(
        [left[:, :reach_cols, :depth], source, right[:, :reach_cols, :depth]], axis=1
    )
    present = jnp.concatenate(
        [
            left[: height + 2, reach_cols:, :channels],
            present,
            right[: height + 2, reach_cols:, :channels],
        ],
        axis=1,
    )
    lane = lax.broadcasted_iota(jnp.int32, (1, 1, depth), 2) // CP
    shifted = None
    for k in range(frames):
        window = lax.dynamic_slice(
            source,
            (reach_rows - 1 - offsets[k, 0], reach_cols - 1 - offsets[k, 1], jnp.int32(0)),
            (height + 2, width + 2, depth),
        )
        shifted = window if shifted is None else jnp.where(lane == k, window, shifted)
    row = lax.broadcasted_iota(jnp.int32, (height + 2, 1, 1), 0) + (
        lax.axis_index("rows") * height - 1
    )
    col = lax.broadcasted_iota(jnp.int32, (1, width + 2, 1), 1) + (
        lax.axis_index("cols") * width - 1
    )
    inside = (row >= 0) & (row < height * lax.axis_size("rows"))
    inside = inside & (col >= 0) & (col < width * lax.axis_size("cols"))
    shifted = jnp.where(inside, shifted, jnp.zeros_like(shifted))
    if SPLIT:
        total = conv(present, mixer_weight[..., :channels])
        total = total + conv(shifted, mixer_weight[..., channels:])
    else:
        total = conv(jnp.concatenate([present, shifted], axis=2), mixer_weight)
    result = jnp.maximum(total + mixer_bias, 0.0).astype(jnp.bfloat16)
    return result.transpose(2, 0, 1)


def solution(mesh):
    in_specs = (P(None, "rows", "cols"), P(None, None, "rows", "cols"), P(), P(), P(), P())
    out_specs = P(None, "rows", "cols")
    return jax.shard_map(body, mesh=mesh, in_specs=in_specs, out_specs=out_specs, check_vma=False)
```
